32 devices in a mesh: seq: 8 (over y, x, core), head: 4 (over z).
Axes of the slice: x: 2, y: 2, z: 4, core: 2. Of those that a mesh axis runs over, the one named last changes fastest.
Arguments:
- queries: bfloat16 [8, 128, 8192], P('seq', None, 'head'), may hold values from -160 to 160
- continuation_key_slots: bfloat16 [8, 128, 1024], P('seq', None, 'head'), may hold values from -13.1875 to 13.1875
- continuation_value_slots: bfloat16 [8, 128, 1024], P('seq', None, 'head'), may hold values from -24 to 24
- cached_prompt_keys: bfloat16 [2, 8192, 1024], P(None, 'seq', 'head'), may hold values from -6 to 6
- cached_prompt_values: bfloat16 [2, 8192, 1024], P(None, 'seq', 'head'), may hold values from -24 to 24
- pair_lengths: int32 [2, 2], replicated, may hold values from 1 to 256
- prompt_of: int32 [2], replicated, may hold values from 0 to 1
- slot_tile: int32 [8], replicated, may hold values from 0 to 7, each once
- out_weight: bfloat16 [8192, 8192], P('head', 'seq'), may hold values from -0.0625 to 0.0625
Outputs:
- projected: bfloat16 [8, 128, 8192], P('head', None, 'seq')
The draws below stay inside these ranges and needn't reach their ends.
Inputs may be any that keep to these rules, and one draw needn't show every extreme that they name: `slot_tile`: each of the 8 tiles stands in exactly one slot.
All inputs are finite; a program needn't handle non-finite values.
Results may differ from the reference program's by a relative error of at most 0.014.
Values may be sent and summed in bfloat16 or wider, within the bound.
A program may use at most 128 MiB of HBM per device.

```python
import math
from functools import partial
import jax
import jax.numpy as jnp
from jax import lax

D = 8192
QUERY_HEADS = 64
KEY_VALUE_HEADS = 8
HEAD_WIDTH = 128
TILE_ROWS = 128
MAX_CONT_TILES = 2
PROMPT_COUNT = 2
TILE_SLOTS = 8
PAIRS = 2
PROMPT_LENGTH = 8192


def prompt_key_block(key):
    sampled_keys = jax.random.truncated_normal(jax.random.fold_in(key, 101), -6.0, 6.0, (PROMPT_COUNT, PROMPT_LENGTH, KEY_VALUE_HEADS * HEAD_WIDTH), jnp.float32)
    return sampled_keys


def draw_cached_prompt_keys(key, part):
    return prompt_key_block(key).astype(jnp.bfloat16)


def draw_queries(key, part):
    drawn = 2.5 * jax.random.truncated_normal(jax.random.fold_in(key, 202), -6.0, 6.0, (TILE_SLOTS, TILE_ROWS, QUERY_HEADS * HEAD_WIDTH), jnp.float32)
    return drawn.astype(jnp.bfloat16)


def plant(values, key, smallest, largest):
    longest = values.shape.index(max(values.shape))
    spots = []
    for shift in (0, 1):
        where = [jax.random.randint(jax.random.fold_in(key, axis), (), 0, length) for axis, length in enumerate(values.shape)]
        where[longest] = (where[longest] + shift) % values.shape[longest]
        spots.append(tuple(where))
    return values.at[spots[0]].set(smallest).at[spots[1]].set(largest)


def levels(rng, extent, cuts, least, largest):
    def one(position, shards_of):
        heights = jax.random.uniform(jax.random.fold_in(jax.random.fold_in(rng, 6), position), (shards_of,), jnp.float32, least / len(cuts), largest / len(cuts))
        return jnp.repeat(jnp.exp(heights), extent[position] // shards_of).reshape((-1,) + (1,) * (len(extent) - position - 1))

    factor_of = one(*cuts[0])
    for cut in cuts[1:]:
        factor_of = factor_of * one(*cut)
    return factor_of


def noise(rng, shape, spread, limit, shards=(), kind=jnp.bfloat16):
    result = spread * jax.random.normal(rng, shape, jnp.float32)
    if shards:
        result = result * levels(rng, shape, shards, -0.22, 0.18)
    return jnp.clip(result, -limit, limit).astype(kind)


def setup_inputs(seed: int = 0) -> dict:
    splits = jax.random.split(jax.random.key(seed), 10)
    queries = draw_queries(jax.random.fold_in(splits[9], 71), 0)
    continuation_key_slots = noise(splits[1], (TILE_SLOTS, TILE_ROWS, KEY_VALUE_HEADS * HEAD_WIDTH), 2.2, 13.1875, ((0, 8), (2, 4)))
    continuation_value_slots = noise(splits[2], (TILE_SLOTS, TILE_ROWS, KEY_VALUE_HEADS * HEAD_WIDTH), 4.0, 24.0, ((0, 8), (2, 4)))
    cached_prompt_keys = draw_cached_prompt_keys(jax.random.fold_in(splits[9], 71), 0)
    cached_prompt_values = noise(splits[4], (PROMPT_COUNT, PROMPT_LENGTH, KEY_VALUE_HEADS * HEAD_WIDTH), 4.0, 24.0, ((1, 8), (2, 4)))
    pair_lengths = plant(jax.random.randint(splits[5], (PAIRS, 2), 1, MAX_CONT_TILES * TILE_ROWS + 1), jax.random.fold_in(splits[5], 1), 1, MAX_CONT_TILES * TILE_ROWS).astype(jnp.int32)
    prompt_of = jax.random.randint(splits[6], (PAIRS,), 0, PROMPT_COUNT).astype(jnp.int32)
    slot_tile = jax.random.permutation(splits[7], TILE_SLOTS).astype(jnp.int32)
    out_weight = noise(splits[8], (QUERY_HEADS * HEAD_WIDTH, D), (QUERY_HEADS * HEAD_WIDTH) ** -0.5, 0.0625, ((0, 4), (1, 8)))
    return {"queries": queries, "continuation_key_slots": continuation_key_slots, "continuation_value_slots": continuation_value_slots, "cached_prompt_keys": cached_prompt_keys, "cached_prompt_values": cached_prompt_values, "pair_lengths": pair_lengths, "prompt_of": prompt_of, "slot_tile": slot_tile, "out_weight": out_weight}


VERY_LOW = -1e+30

def round_weights(weights):
    rounded = lax.optimization_barrier(weights.astype(jnp.bfloat16))
    return rounded.astype(jnp.float32)

def group_attention(items, causal, scaling):
    query_group, prompt_key_rows, prompt_value_rows, self_key_block, self_value_block = items
    prompt_scores = jnp.einsum('tgd,pd->gtp', query_group, prompt_key_rows, precision=lax.Precision.HIGHEST) * scaling
    own_scores = jnp.einsum('tgd,pd->gtp', query_group, self_key_block, precision=lax.Precision.HIGHEST) * scaling
    own_scores = jnp.where(causal[None], own_scores, VERY_LOW)
    peak = jnp.maximum(lax.optimization_barrier(jnp.max(prompt_scores, axis=2)), lax.optimization_barrier(jnp.max(own_scores, axis=2)))
    prompt_w = jnp.exp(prompt_scores - peak[:, :, None])
    own_w = jnp.exp(own_scores - peak[:, :, None])
    denominator = lax.optimization_barrier(jnp.sum(prompt_w, axis=2)) + lax.optimization_barrier(jnp.sum(own_w, axis=2))
    numerator = jnp.einsum('gtp,pd->gtd', round_weights(prompt_w), prompt_value_rows, precision=lax.Precision.HIGHEST)
    numerator = numerator + jnp.einsum('gtp,pd->gtd', round_weights(own_w), self_value_block, precision=lax.Precision.HIGHEST)
    return numerator / denominator[:, :, None]

def reference(queries, continuation_key_slots, continuation_value_slots, cached_prompt_keys, cached_prompt_values, pair_lengths, prompt_of, slot_tile, out_weight):
    scaling = 1.0 / math.sqrt(HEAD_WIDTH)
    owner_slot = jnp.zeros((TILE_SLOTS,), jnp.int32).at[slot_tile].set(jnp.arange(TILE_SLOTS, dtype=jnp.int32))
    lengths = pair_lengths.reshape(2 * PAIRS)

    def one_slot(slot_index):
        tile_id = slot_tile[slot_index]
        continuation = tile_id // MAX_CONT_TILES
        offset = tile_id % MAX_CONT_TILES * TILE_ROWS
        prompt_index = prompt_of[continuation // 2]
        prompt_key_rows = lax.dynamic_index_in_dim(cached_prompt_keys, prompt_index, 0, False).astype(jnp.float32).reshape(PROMPT_LENGTH, KEY_VALUE_HEADS, HEAD_WIDTH)
        prompt_value_rows = lax.dynamic_index_in_dim(cached_prompt_values, prompt_index, 0, False).astype(jnp.float32).reshape(PROMPT_LENGTH, KEY_VALUE_HEADS, HEAD_WIDTH)
        place_indices = owner_slot[continuation * MAX_CONT_TILES + jnp.arange(MAX_CONT_TILES, dtype=jnp.int32)]
        self_key_block = continuation_key_slots[place_indices].astype(jnp.float32).reshape(MAX_CONT_TILES * TILE_ROWS, KEY_VALUE_HEADS, HEAD_WIDTH)
        self_value_block = continuation_value_slots[place_indices].astype(jnp.float32).reshape(MAX_CONT_TILES * TILE_ROWS, KEY_VALUE_HEADS, HEAD_WIDTH)
        query_vectors = lax.dynamic_index_in_dim(queries, slot_index, 0, False).astype(jnp.float32).reshape(TILE_ROWS, KEY_VALUE_HEADS, QUERY_HEADS // KEY_VALUE_HEADS, HEAD_WIDTH)
        row_pos = offset + jnp.arange(TILE_ROWS, dtype=jnp.int32)
        col_pos = jnp.arange(MAX_CONT_TILES * TILE_ROWS, dtype=jnp.int32)
        causal = col_pos[None, :] <= row_pos[:, None]
        in_length = row_pos < lengths[continuation]
        per_head = lax.map(partial(group_attention, causal=causal, scaling=scaling), (jnp.moveaxis(query_vectors, 1, 0), jnp.moveaxis(prompt_key_rows, 1, 0), jnp.moveaxis(prompt_value_rows, 1, 0), jnp.moveaxis(self_key_block, 1, 0), jnp.moveaxis(self_value_block, 1, 0)))
        per_head = jnp.transpose(per_head, (2, 0, 1, 3)).reshape(TILE_ROWS, QUERY_HEADS * HEAD_WIDTH)
        return jnp.where(in_length[:, None], per_head, 0.0).astype(jnp.bfloat16)
    attention = lax.map(one_slot, jnp.arange(TILE_SLOTS, dtype=jnp.int32))
    projected = jnp.dot(attention.reshape(TILE_SLOTS * TILE_ROWS, QUERY_HEADS * HEAD_WIDTH), out_weight, preferred_element_type=jnp.float32)
    return projected.astype(jnp.bfloat16).reshape(TILE_SLOTS, TILE_ROWS, D)
```

```python
import functools
import math

import jax
import jax.numpy as jnp
from jax import lax
from jax.experimental import pallas as pl
from jax.experimental.pallas import tpu as pltpu
from jax.sharding import PartitionSpec as P

QUERY_HEADS = 64
KEY_VALUE_HEADS = 8
HEAD_WIDTH = 128
TILE_ROWS = 128
MAX_CONT_TILES = 2
GROUP = QUERY_HEADS // KEY_VALUE_HEADS
LANES = 128
HALF = LANES // 2
VERY_LOW = -1e30
MESH = pl.DeviceIdType.MESH
EXP2_SCALE = math.log2(math.e) / math.sqrt(HEAD_WIDTH)


def flip(index, mask):
    return index + mask * (1 - 2 * (lax.rem(index // mask, 2)))


def chip_mask(step, core, bits):
    which = lax.rem(step + core, bits)
    return 2 * (1 + which + which * (which - 1) // 2)


def kernel(
    n,
    peers,
    q_hbm,
    kc_ref,
    vc_ref,
    k_ref,
    v_ref,
    lengths_ref,
    prompt_ref,
    tile_ref,
    w_hbm,
    out_ref,
    q_all,
    o_all,
    stats,
    o_core,
    st_core,
    o_chip,
    st_chip,
    attn,
    w_ref,
    share,
    arrived,
    local_sem,
    send_sem,
    recv_sem,
    z_send,
    z_recv,
):
    me = lax.axis_index("seq")
    z = lax.axis_index("head")
    core = lax.rem(me, 2)
    partner = flip(me, 1)
    half = n // 2
    bits = half.bit_length() - 1
    heads = q_hbm.shape[-1] // HEAD_WIDTH
    per_z = n // peers
    masks = [chip_mask(step, core, bits) for step in range(bits)]
    partner_masks = [chip_mask(step, 1 - core, bits) for step in range(bits)]
    mine, theirs = [me], [partner]
    for step in range(bits):
        mine += [flip(slot, masks[step]) for slot in mine]
        theirs += [flip(slot, partner_masks[step]) for slot in theirs]

    q_load = pltpu.make_async_copy(q_hbm.at[0], q_all.at[me], local_sem.at[0])
    w_load = pltpu.make_async_copy(w_hbm, w_ref, local_sem.at[1])
    q_load.start()
    w_load.start()
    barrier = pltpu.get_barrier_semaphore()
    neighbours = [(partner, z)] + [(flip(me, mask), z) for mask in masks]
    neighbours += [(me, lax.rem(z + hop, peers)) for hop in range(1, peers)]
    for device in neighbours:
        pl.semaphore_signal(barrier, inc=1, device_id=device, device_id_type=MESH)
    pl.semaphore_wait(barrier, len(neighbours))
    q_load.wait()

    counter = [0]
    sent = []

    def remote(src, dst, seq):
        index = counter[0]
        counter[0] += 1
        copy = pltpu.make_async_remote_copy(
            src_ref=src,
            dst_ref=dst,
            send_sem=send_sem.at[index],
            recv_sem=recv_sem.at[index],
            device_id=(seq, z),
            device_id_type=MESH,
        )
        sent.append(copy)
        return copy

    def gather(buf, use, flush):
        links = [
            [remote(buf.at[mine[j]], buf.at[mine[j]], flip(me, masks[step])) for j in range(2**step)]
            for step in range(bits)
        ]
        cores = [remote(buf.at[mine[j]], buf.at[mine[j]], partner) for j in range(half)]
        if bits:
            links[0][0].start()
        cores[0].start()
        use(mine[0])
        for step in range(1, bits):
            links[step][0].start()
        cores[0].wait_recv()
        use(theirs[0])
        flush(0)
        for step in range(bits):
            for j in range(2**step):
                slot = 2**step + j
                links[step][j].wait_recv()
                cores[slot].start()
                for later in range(step + 1, bits):
                    links[later][slot].start()
                use(mine[slot])
                cores[slot].wait_recv()
                use(theirs[slot])
                flush(slot)

    lane = lax.broadcasted_iota(jnp.int32, (TILE_ROWS, LANES), 1)
    row = lax.broadcasted_iota(jnp.int32, (TILE_ROWS, LANES), 0)
    own_tile = tile_ref[me]

    def attend(slot):
        tile = tile_ref[slot]
        prompt = prompt_ref[tile // MAX_CONT_TILES // 2]
        same = (tile // MAX_CONT_TILES) == (own_tile // MAX_CONT_TILES)
        shift = (tile % MAX_CONT_TILES - own_tile % MAX_CONT_TILES) * TILE_ROWS
        shift = jnp.where(same, shift, -1000000)
        allowed = (lane - row) <= shift
        allowed = jnp.concatenate([allowed.astype(jnp.float32)] * 2, axis=0) > 0.5
        stats[slot] = jnp.ones((TILE_ROWS, LANES), jnp.float32)
        contract = (((1,), (1,)), ((), ()))

        def block(step, carry):
            kv = (step * 4) // GROUP
            kv_lanes = pl.ds(pl.multiple_of(kv * HEAD_WIDTH, HEAD_WIDTH), HEAD_WIDTH)
            for part in range(2):
                head = step * 4 + part * 2
                lanes = [
                    pl.ds(pl.multiple_of((head + i) * HEAD_WIDTH, HEAD_WIDTH), HEAD_WIDTH)
                    for i in range(2)
                ]
                query = jnp.concatenate([q_all[slot, :, where] for where in lanes], axis=0)
                raw = lax.dot_general(
                    query, k_ref[prompt, :, kv_lanes], contract, preferred_element_type=jnp.float32
                )
                raw_own = lax.dot_general(
                    query, kc_ref[0, :, kv_lanes], contract, preferred_element_type=jnp.float32
                )
                raw_own = jnp.where(allowed, raw_own, VERY_LOW)
                peak = jnp.maximum(
                    jnp.max(raw, axis=1, keepdims=True), jnp.max(raw_own, axis=1, keepdims=True)
                )
                weights = jnp.exp2((raw - peak) * EXP2_SCALE).astype(jnp.bfloat16)
                weights_own = jnp.exp2((raw_own - peak) * EXP2_SCALE).astype(jnp.bfloat16)
                values = v_ref[prompt, :, kv_lanes]
                values_own = vc_ref[0, :, kv_lanes]
                both = jnp.dot(
                    weights,
                    jnp.concatenate([values, jnp.ones_like(values)], axis=1),
                    preferred_element_type=jnp.float32,
                ) + jnp.dot(
                    weights_own,
                    jnp.concatenate([values_own, jnp.ones_like(values_own)], axis=1),
                    preferred_element_type=jnp.float32,
                )
                total = both[:, HEAD_WIDTH:]
                out = (both[:, :HEAD_WIDTH] / total).astype(jnp.bfloat16)
                tile_stats = stats[slot]
                for i in range(2):
                    rows = slice(i * TILE_ROWS, (i + 1) * TILE_ROWS)
                    o_all[slot, :, lanes[i]] = out[rows]
                    tile_stats = jnp.where(lane == head + i, peak[rows], tile_stats)
                    tile_stats = jnp.where(lane == HALF + head + i, total[rows], tile_stats)
                stats[slot] = tile_stats
            return carry

        lax.fori_loop(0, heads // 4, block, 0)

    def merge(slot, other_o, other_st, store):
        one, two = stats[slot], other_st[...]
        top = jnp.maximum(one, two)
        share_one = jnp.exp2((one - top) * EXP2_SCALE) * pltpu.roll(one, HALF, 1)
        share_two = jnp.exp2((two - top) * EXP2_SCALE) * pltpu.roll(two, HALF, 1)
        total = share_one + share_two
        stats[slot] = jnp.where(lane < HALF, top, pltpu.roll(total, HALF, 1))
        share_one = share_one / total
        share_two = share_two / total
        for head in range(heads):
            lanes = slice(head * HEAD_WIDTH, (head + 1) * HEAD_WIDTH)
            store(
                lanes,
                o_all[slot, :, lanes].astype(jnp.float32) * share_one[:, head : head + 1]
                + other_o[:, lanes].astype(jnp.float32) * share_two[:, head : head + 1],
            )

    def keep(slot):
        def store(lanes, value):
            o_all[slot, :, lanes] = value.astype(jnp.bfloat16)

        return store

    to_core = []

    def attend_and_send(slot):
        attend(slot)

    def flush_core(j):
        del j

    def use_query(slot):
        attend(slot)
        if any(slot is other for other in theirs):
            j = [slot is other for other in theirs].index(True)
            pair = (
                remote(o_all.at[slot], o_core.at[j], partner),
                remote(stats.at[slot], st_core.at[j], partner),
            )
            for copy in pair:
                copy.start()
            to_core.append(pair)

    chip = {}

    def start_chip(step, j):
        slot = mine[2**step + j]
        base = 2**step - 1 + j
        pair = (
            remote(o_all.at[slot], o_chip.at[base], flip(me, masks[step])),
            remote(stats.at[slot], st_chip.at[base], flip(me, masks[step])),
        )
        for copy in pair:
            copy.start()
        chip[step, j] = pair

    def merge_core(j):
        for copy in to_core[j]:
            copy.wait_recv()
        merge(mine[j], o_core.at[j], st_core.at[j], keep(mine[j]))
        if bits and j >= 2 ** (bits - 1):
            start_chip(bits - 1, j - 2 ** (bits - 1))

    gather(q_all, use_query, merge_core)

    tile = own_tile
    continuation = tile // MAX_CONT_TILES
    length = lengths_ref[continuation // 2, continuation % 2]
    in_length = (tile % MAX_CONT_TILES) * TILE_ROWS + row < length

    def finish(lanes, value):
        attn[me, :, lanes] = jnp.where(in_length, value, 0.0).astype(jnp.bfloat16)

    for step in reversed(range(bits)):
        for j in reversed(range(2**step)):
            for copy in chip[step, j]:
                copy.wait_recv()
            base = 2**step - 1 + j
            last = step == 0
            merge(mine[j], o_chip.at[base], st_chip.at[base], finish if last else keep(mine[j]))
            if step and j >= 2 ** (step - 1):
                start_chip(step - 1, j - 2 ** (step - 1))

    w_load.wait()
    pending = []
    z_sent = []

    def use_attention(slot):
        pending.append(slot)

    def project(j):
        del j
        slots = [pending.pop(0), pending.pop(0)]
        rows = jnp.concatenate([attn[slot] for slot in slots], axis=0)
        product = jnp.dot(rows, w_ref[...], preferred_element_type=jnp.float32)
        product = product.astype(jnp.bfloat16)
        for i, slot in enumerate(slots):
            share[slot] = product[i * TILE_ROWS : (i + 1) * TILE_ROWS]
            owner, place = slot // per_z, lax.rem(slot, per_z)
            copy = pltpu.make_async_remote_copy(
                src_ref=share.at[slot],
                dst_ref=arrived.at[z, place],
                send_sem=z_send.at[slot],
                recv_sem=z_recv.at[z, place],
                device_id=(me, owner),
                device_id_type=MESH,
            )

            @pl.when(owner != z)
            def _(copy=copy):
                copy.start()

            z_sent.append((owner, copy))

    gather(attn, use_attention, project)

    totals = [share[z * per_z + place].astype(jnp.float32) for place in range(per_z)]
    for hop in range(1, peers):
        source = lax.rem(z + hop, peers)
        for place in range(per_z):
            pltpu.make_async_remote_copy(
                src_ref=share.at[z * per_z + place],
                dst_ref=arrived.at[source, place],
                send_sem=z_send.at[z * per_z + place],
                recv_sem=z_recv.at[source, place],
                device_id=(me, source),
                device_id_type=MESH,
            ).wait_recv()
            totals[place] += arrived[source, place].astype(jnp.float32)
    for place in range(per_z):
        out_ref[place] = totals[place].astype(out_ref.dtype)
    for copy in sent:
        copy.wait_send()
    for owner, copy in z_sent:

        @pl.when(owner != z)
        def _(copy=copy):
            copy.wait_send()


def local(n, peers, queries, kc, vc, keys, values, pair_lengths, prompt_of, slot_tile, out_weight):
    features = queries.shape[-1]
    columns = out_weight.shape[-1]
    half = n // 2
    bits = half.bit_length() - 1
    gathers = 2 * (half - 1 + half)
    copies = gathers + 2 * half + 2 * (half - 1)
    vmem = pl.BlockSpec(memory_space=pltpu.VMEM)
    smem = pl.BlockSpec(memory_space=pltpu.SMEM)
    hbm = pl.BlockSpec(memory_space=pl.ANY)
    slot = (TILE_ROWS, features)
    stat = (TILE_ROWS, LANES)
    scratch = [
        pltpu.VMEM((n, *slot), jnp.bfloat16),
        pltpu.VMEM((n, *slot), jnp.bfloat16),
        pltpu.VMEM((n, *stat), jnp.float32),
        pltpu.VMEM((half, *slot), jnp.bfloat16),
        pltpu.VMEM((half, *stat), jnp.float32),
        pltpu.VMEM((half, *slot), jnp.bfloat16),
        pltpu.VMEM((half, *stat), jnp.float32),
        pltpu.VMEM((n, *slot), jnp.bfloat16),
        pltpu.VMEM(out_weight.shape, jnp.bfloat16),
        pltpu.VMEM((n, TILE_ROWS, columns), jnp.bfloat16),
        pltpu.VMEM((peers, n // peers, TILE_ROWS, columns), jnp.bfloat16),
        pltpu.SemaphoreType.DMA((2,)),
        pltpu.SemaphoreType.DMA((copies,)),
        pltpu.SemaphoreType.DMA((copies,)),
        pltpu.SemaphoreType.DMA((n,)),
        pltpu.SemaphoreType.DMA((peers, n // peers)),
    ]
    return pl.pallas_call(
        functools.partial(kernel, n, peers),
        out_shape=jax.ShapeDtypeStruct((n // peers, TILE_ROWS, columns), jnp.bfloat16),
        in_specs=[hbm, vmem, vmem, vmem, vmem, smem, smem, smem, hbm],
        out_specs=vmem,
        scratch_shapes=scratch,
        compiler_params=pltpu.CompilerParams(
            collective_id=0, has_side_effects=True, vmem_limit_bytes=60 * 1024 * 1024
        ),
    )(queries, kc, vc, keys, values, pair_lengths, prompt_of, slot_tile, out_weight)


def solution(mesh):
    return jax.shard_map(
        functools.partial(local, mesh.shape["seq"], mesh.shape["head"]),
        mesh=mesh,
        in_specs=(
            P("seq", None, "head"),
            P("seq", None, "head"),
            P("seq", None, "head"),
            P(None, "seq", "head"),
            P(None, "seq", "head"),
            P(),
            P(),
            P(),
            P("head", "seq"),
        ),
        out_specs=P("head", None, "seq"),
        check_vma=False,
    )
```

```python
import functools
import math

import jax
import jax.numpy as jnp
from jax import lax
from jax.experimental import pallas as pl
from jax.experimental.pallas import tpu as pltpu
from jax.sharding import PartitionSpec as P

QUERY_HEADS = 64
KEY_VALUE_HEADS = 8
HEAD_WIDTH = 128
TILE_ROWS = 128
PARTS = 2
PART_ROWS = TILE_ROWS // PARTS
STACK = 4
MAX_CONT_TILES = 2
GROUP = QUERY_HEADS // KEY_VALUE_HEADS
LANES = 128
HALF = LANES // 2
VERY_LOW = -1e30
MESH = pl.DeviceIdType.MESH
EXP2_SCALE = math.log2(math.e) / math.sqrt(HEAD_WIDTH)


def flip(index, mask):
    return index + mask * (1 - 2 * (lax.rem(index // mask, 2)))


def chip_mask(step, core, bits):
    which = lax.rem(step + core, bits)
    return 2 * (1 + which + which * (which - 1) // 2)


def kernel(
    n,
    peers,
    q_hbm,
    kc_ref,
    vc_ref,
    k_ref,
    v_ref,
    lengths_ref,
    prompt_ref,
    tile_ref,
    w_hbm,
    out_ref,
    q_all,
    o_all,
    stats,
    o_core,
    st_core,
    o_chip,
    st_chip,
    attn,
    w_ref,
    share,
    arrived,
    local_sem,
    send_sem,
    recv_sem,
    z_send,
    z_recv,
):
    me = lax.axis_index("seq")
    z = lax.axis_index("head")
    core = lax.rem(me, 2)
    partner = flip(me, 1)
    half = n // 2
    bits = half.bit_length() - 1
    heads = q_hbm.shape[-1] // HEAD_WIDTH
    per_z = n // peers
    masks = [chip_mask(step, core, bits) for step in range(bits)]
    partner_masks = [chip_mask(step, 1 - core, bits) for step in range(bits)]
    mine, theirs = [me], [partner]
    for step in range(bits):
        mine += [flip(slot, masks[step]) for slot in mine]
        theirs += [flip(slot, partner_masks[step]) for slot in theirs]

    q_load = pltpu.make_async_copy(q_hbm.at[0], q_all.at[me], local_sem.at[0])
    w_load = pltpu.make_async_copy(w_hbm, w_ref, local_sem.at[1])
    q_load.start()
    w_load.start()
    barrier = pltpu.get_barrier_semaphore()
    neighbours = [(partner, z)] + [(flip(me, mask), z) for mask in masks]
    neighbours += [(me, lax.rem(z + hop, peers)) for hop in range(1, peers)]
    for device in neighbours:
        pl.semaphore_signal(barrier, inc=1, device_id=device, device_id_type=MESH)
    pl.semaphore_wait(barrier, len(neighbours))
    q_load.wait()

    counter = [0]
    sent = []

    def remote(src, dst, seq):
        index = counter[0]
        counter[0] += 1
        copy = pltpu.make_async_remote_copy(
            src_ref=src,
            dst_ref=dst,
            send_sem=send_sem.at[index],
            recv_sem=recv_sem.at[index],
            device_id=(seq, z),
            device_id_type=MESH,
        )
        sent.append(copy)
        return copy

    lane = lax.broadcasted_iota(jnp.int32, (PART_ROWS, LANES), 1)
    row = lax.broadcasted_iota(jnp.int32, (PART_ROWS, LANES), 0)
    own_tile = tile_ref[me]

    def attend(slot, part):
        rows = slice(part * PART_ROWS, (part + 1) * PART_ROWS)
        tile = tile_ref[slot]
        prompt = prompt_ref[tile // MAX_CONT_TILES // 2]
        same = (tile // MAX_CONT_TILES) == (own_tile // MAX_CONT_TILES)
        shift = (tile % MAX_CONT_TILES - own_tile % MAX_CONT_TILES) * TILE_ROWS
        shift = jnp.where(same, shift + part * PART_ROWS, -1000000)
        allowed = (lane - row) <= shift
        allowed = jnp.concatenate([allowed.astype(jnp.float32)] * STACK, axis=0) > 0.5
        stats[slot, rows] = jnp.ones((PART_ROWS, LANES), jnp.float32)
        contract = (((1,), (1,)), ((), ()))

        def block(kv, carry):
            kv_lanes = pl.ds(pl.multiple_of(kv * HEAD_WIDTH, HEAD_WIDTH), HEAD_WIDTH)
            for first in range(0, GROUP, STACK):
                head = kv * GROUP + first
                lanes = [
                    pl.ds(pl.multiple_of((head + i) * HEAD_WIDTH, HEAD_WIDTH), HEAD_WIDTH)
                    for i in range(STACK)
                ]
                query = jnp.concatenate([q_all[slot, rows, where] for where in lanes], axis=0)
                raw = lax.dot_general(
                    query, k_ref[prompt, :, kv_lanes], contract, preferred_element_type=jnp.float32
                )
                raw_own = lax.dot_general(
                    query, kc_ref[0, :, kv_lanes], contract, preferred_element_type=jnp.float32
                )
                raw_own = jnp.where(allowed, raw_own, VERY_LOW)
                peak = jnp.maximum(
                    jnp.max(raw, axis=1, keepdims=True), jnp.max(raw_own, axis=1, keepdims=True)
                )
                weights = jnp.exp2((raw - peak) * EXP2_SCALE).astype(jnp.bfloat16)
                weights_own = jnp.exp2((raw_own - peak) * EXP2_SCALE).astype(jnp.bfloat16)
                values = v_ref[prompt, :, kv_lanes]
                values_own = vc_ref[0, :, kv_lanes]
                both = jnp.dot(
                    weights,
                    jnp.concatenate([values, jnp.ones_like(values)], axis=1),
                    preferred_element_type=jnp.float32,
                ) + jnp.dot(
                    weights_own,
                    jnp.concatenate([values_own, jnp.ones_like(values_own)], axis=1),
                    preferred_element_type=jnp.float32,
                )
                total = both[:, HEAD_WIDTH:]
                out = (both[:, :HEAD_WIDTH] / total).astype(jnp.bfloat16)
                tile_stats = stats[slot, rows]
                for i in range(STACK):
                    of = slice(i * PART_ROWS, (i + 1) * PART_ROWS)
                    o_all[slot, rows, lanes[i]] = out[of]
                    tile_stats = jnp.where(lane == head + i, peak[of], tile_stats)
                    tile_stats = jnp.where(lane == HALF + head + i, total[of], tile_stats)
                stats[slot, rows] = tile_stats
            return carry

        lax.fori_loop(0, heads // GROUP, block, 0)

    class Part:
        def __init__(self, part):
            self.part = part
            self.rows = slice(part * PART_ROWS, (part + 1) * PART_ROWS)
            self.at = pl.ds(part * PART_ROWS, PART_ROWS)
            self.to_core = []
            self.chip = {}
            self.queries = self.routes(q_all)

        def routes(self, buf):
            def route(slot, seq):
                ref = buf.at[slot, self.at]
                return remote(ref, ref, seq)

            links = [
                [route(mine[j], flip(me, masks[step])) for j in range(2**step)]
                for step in range(bits)
            ]
            return links, [route(mine[j], partner) for j in range(half)]

        def begin(self, routes):
            links, cores = routes
            for step in range(bits):
                links[step][0].start()
            cores[0].start()

        def forward(self, routes, slot):
            links, cores = routes
            step = slot.bit_length() - 1
            links[step][slot - 2**step].wait_recv()
            cores[slot].start()
            for later in range(step + 1, bits):
                links[later][slot].start()

        def score(self, j):
            self.queries[1][j].wait_recv()
            attend(theirs[j], self.part)
            pair = (
                remote(o_all.at[theirs[j], self.at], o_core.at[j, self.at], partner),
                remote(stats.at[theirs[j], self.at], st_core.at[j, self.at], partner),
            )
            for copy in pair:
                copy.start()
            attend(mine[j], self.part)
            for copy in pair:
                copy.wait_recv()
            self.merge(mine[j], o_core, st_core, j, self.keep(mine[j]))
            if bits and j >= 2 ** (bits - 1):
                self.start_chip(bits - 1, j - 2 ** (bits - 1))

        def start_chip(self, step, j):
            slot = mine[2**step + j]
            base = 2**step - 1 + j
            to = flip(me, masks[step])
            pair = (
                remote(o_all.at[slot, self.at], o_chip.at[base, self.at], to),
                remote(stats.at[slot, self.at], st_chip.at[base, self.at], to),
            )
            for copy in pair:
                copy.start()
            self.chip[step, j] = pair

        def merge(self, slot, other_o, other_st, place, store):
            one, two = stats[slot, self.rows], other_st[place, self.rows]
            top = jnp.maximum(one, two)
            share_one = jnp.exp2((one - top) * EXP2_SCALE) * pltpu.roll(one, HALF, 1)
            share_two = jnp.exp2((two - top) * EXP2_SCALE) * pltpu.roll(two, HALF, 1)
            total = share_one + share_two
            stats[slot, self.rows] = jnp.where(lane < HALF, top, pltpu.roll(total, HALF, 1))
            share_one = share_one / total
            share_two = share_two / total
            for head in range(heads):
                lanes = slice(head * HEAD_WIDTH, (head + 1) * HEAD_WIDTH)
                store(
                    lanes,
                    o_all[slot, self.rows, lanes].astype(jnp.float32)
                    * share_one[:, head : head + 1]
                    + other_o[place, self.rows, lanes].astype(jnp.float32)
                    * share_two[:, head : head + 1],
                )

        def keep(self, slot):
            def store(lanes, value):
                o_all[slot, self.rows, lanes] = value.astype(jnp.bfloat16)

            return store

        def finish(self, lanes, value):
            continuation = own_tile // MAX_CONT_TILES
            length = lengths_ref[continuation // 2, continuation % 2]
            first = (own_tile % MAX_CONT_TILES) * TILE_ROWS + self.part * PART_ROWS
            value = jnp.where(first + row < length, value, 0.0)
            attn[me, self.rows, lanes] = value.astype(jnp.bfloat16)

        def project(self, slots):
            rows = jnp.concatenate([attn[slot, self.rows] for slot in slots], axis=0)
            product = jnp.dot(rows, w_ref[...], preferred_element_type=jnp.float32)
            product = product.astype(jnp.bfloat16)
            for i, slot in enumerate(slots):
                share[slot, self.rows] = product[i * PART_ROWS : (i + 1) * PART_ROWS]
                owner, place = slot // per_z, lax.rem(slot, per_z)
                copy = pltpu.make_async_remote_copy(
                    src_ref=share.at[slot, self.at],
                    dst_ref=arrived.at[z, place, self.at],
                    send_sem=z_send.at[self.part, slot],
                    recv_sem=z_recv.at[self.part, z, place],
                    device_id=(me, owner),
                    device_id_type=MESH,
                )

                @pl.when(owner != z)
                def _(copy=copy):
                    copy.start()

                z_sent.append((owner, copy))

        def after(self):
            for step in reversed(range(bits)):
                for j in reversed(range(2**step)):
                    for copy in self.chip[step, j]:
                        copy.wait_recv()
                    base = 2**step - 1 + j
                    store = self.finish if step == 0 else self.keep(mine[j])
                    self.merge(mine[j], o_chip, st_chip, base, store)
                    if step and j >= 2 ** (step - 1):
                        self.start_chip(step - 1, j - 2 ** (step - 1))
                if step:
                    yield
            routes = self.routes(attn)
            self.begin(routes)
            if self.part == 0:
                w_load.wait()
            yield
            slots = []
            for slot in range(half):
                if slot:
                    self.forward(routes, slot)
                    yield
                routes[1][slot].wait_recv()
                slots += [mine[slot], theirs[slot]]
                if True:
                    self.project(slots)
                    slots = []
                    yield

        def collect(self):
            totals = [
                share[z * per_z + place, self.rows].astype(jnp.float32) for place in range(per_z)
            ]
            for hop in range(1, peers):
                source = lax.rem(z + hop, peers)
                for place in range(per_z):
                    pltpu.make_async_remote_copy(
                        src_ref=share.at[z * per_z + place, self.at],
                        dst_ref=arrived.at[source, place, self.at],
                        send_sem=z_send.at[self.part, z * per_z + place],
                        recv_sem=z_recv.at[self.part, source, place],
                        device_id=(me, source),
                        device_id_type=MESH,
                    ).wait_recv()
                    totals[place] += arrived[source, place, self.rows].astype(jnp.float32)
            for place in range(per_z):
                out_ref[place, self.rows] = totals[place].astype(out_ref.dtype)

    z_sent = []
    early, late = Part(0), Part(1)
    early.begin(early.queries)
    late.begin(late.queries)
    early.score(0)
    for slot in range(1, half):
        early.forward(early.queries, slot)
        early.score(slot)
        late.forward(late.queries, slot)
    early_after, late_after = early.after(), late.after()
    for slot in range(half):
        late.score(slot)
        if slot:
            next(early_after, None)
    running = [early_after, late_after]
    while running:
        for one in list(running):
            try:
                next(one)
            except StopIteration:
                running.remove(one)
    early.collect()
    late.collect()
    for copy in sent:
        copy.wait_send()
    for owner, copy in z_sent:

        @pl.when(owner != z)
        def _(copy=copy):
            copy.wait_send()


def local(n, peers, queries, kc, vc, keys, values, pair_lengths, prompt_of, slot_tile, out_weight):
    features = queries.shape[-1]
    columns = out_weight.shape[-1]
    half = n // 2
    bits = half.bit_length() - 1
    gathers = 2 * (half - 1 + half)
    copies = PARTS * (gathers + 2 * half + 2 * (half - 1))
    vmem = pl.BlockSpec(memory_space=pltpu.VMEM)
    smem = pl.BlockSpec(memory_space=pltpu.SMEM)
    hbm = pl.BlockSpec(memory_space=pl.ANY)
    slot = (TILE_ROWS, features)
    stat = (TILE_ROWS, LANES)
    scratch = [
        pltpu.VMEM((n, *slot), jnp.bfloat16),
        pltpu.VMEM((n, *slot), jnp.bfloat16),
        pltpu.VMEM((n, *stat), jnp.float32),
        pltpu.VMEM((half, *slot), jnp.bfloat16),
        pltpu.VMEM((half, *stat), jnp.float32),
        pltpu.VMEM((half, *slot), jnp.bfloat16),
        pltpu.VMEM((half, *stat), jnp.float32),
        pltpu.VMEM((n, *slot), jnp.bfloat16),
        pltpu.VMEM(out_weight.shape, jnp.bfloat16),
        pltpu.VMEM((n, TILE_ROWS, columns), jnp.bfloat16),
        pltpu.VMEM((peers, n // peers, TILE_ROWS, columns), jnp.bfloat16),
        pltpu.SemaphoreType.DMA((2,)),
        pltpu.SemaphoreType.DMA((copies,)),
        pltpu.SemaphoreType.DMA((copies,)),
        pltpu.SemaphoreType.DMA((PARTS, n)),
        pltpu.SemaphoreType.DMA((PARTS, peers, n // peers)),
    ]
    return pl.pallas_call(
        functools.partial(kernel, n, peers),
        out_shape=jax.ShapeDtypeStruct((n // peers, TILE_ROWS, columns), jnp.bfloat16),
        in_specs=[hbm, vmem, vmem, vmem, vmem, smem, smem, smem, hbm],
        out_specs=vmem,
        scratch_shapes=scratch,
        compiler_params=pltpu.CompilerParams(
            collective_id=0, has_side_effects=True, vmem_limit_bytes=60 * 1024 * 1024
        ),
    )(queries, kc, vc, keys, values, pair_lengths, prompt_of, slot_tile, out_weight)


def solution(mesh):
    return jax.shard_map(
        functools.partial(local, mesh.shape["seq"], mesh.shape["head"]),
        mesh=mesh,
        in_specs=(
            P("seq", None, "head"),
            P("seq", None, "head"),
            P("seq", None, "head"),
            P(None, "seq", "head"),
            P(None, "seq", "head"),
            P(),
            P(),
            P(),
            P("head", "seq"),
        ),
        out_specs=P("head", None, "seq"),
        check_vma=False,
    )
```
